32 devices in a mesh: dp: 4 (over y, x), expert: 8 (over z, core).
Axes of the slice: x: 2, y: 2, z: 4, core: 2. Of those that a mesh axis runs over, the one named last changes fastest.
Arguments:
- hidden_in: bfloat16 [8192, 1024], P(('dp', 'expert')), may hold values from -6 to 6
- moe_gain: float32 [1024], replicated, may hold values from 0.1 to 1.9
- router_weight: bfloat16 [1024, 16], replicated, may hold values from -0.1875 to 0.1875
- expert_gate: bfloat16 [16, 1024, 1024], P('expert'), may hold values from -0.1875 to 0.1875
- expert_up: bfloat16 [16, 1024, 1024], P('expert'), may hold values from -0.1875 to 0.1875
- expert_down: bfloat16 [16, 1024, 1024], P('expert'), may hold values from -0.1875 to 0.1875
- final_gain: float32 [1024], replicated, may hold values from 0.1 to 1.9
- vocab_weight: bfloat16 [1024, 32768], P(None, 'expert'), may hold values from -24 to 24
- token_ids: int32 [8192], P(('dp', 'expert')), may hold values from 0 to 32767
- doc_ids: int32 [8192], P(('dp', 'expert')), may hold values from 0 to 127, as said below
- routes: int32 [8192, 2], P(('dp', 'expert')), may hold values from 0 to 15, all different within a row; in each aligned block of 256 rows (0 to 255, 256 to 511, ...) at most 64 rows name the same one
Outputs:
- token_loss: float32 [8192], P(('dp', 'expert'))
- doc_score: float32 [128], P(('dp', 'expert'))
The draws below stay inside these ranges and needn't reach their ends.
Inputs may be any that keep to these rules, and one draw needn't show every extreme that they name: `routes`: among the rows of one device no expert is named more than 64 times; in every draw some expert is named exactly 64 times by the rows of some device. `doc_ids`: documents are numbered in the order of the stream; each document is one run of consecutive tokens, shorter than 512; every document number is used; the rows of each device hold the first tokens of exactly 4 documents.
All inputs are finite; a program needn't handle non-finite values.
Results may differ from the reference program's by a relative error of at most 0.0031.
Values may be sent and summed in bfloat16 or wider, within the bound.
No kernel may reach another device: no remote copies, remote signals or barrier semaphores. Data moves between devices by JAX's collectives and lax.ppermute only.
A program may use at most 128 MiB of HBM per device.

```python
import math
import jax
import jax.numpy as jnp
import numpy as np
from jax import lax

D = 1024
FF = 1024
V = 32768
TOP = 2
E = 16
TOK_DEV = 256
TOKENS = 8192
CAP = 64
DOC_DEV = 4
DOCS = 128
N_DP = 4
N_EXPERT = 8


def draw_vocab_weight(key, part):
    first_key = jax.random.fold_in(jax.random.fold_in(key, 7), 0)
    values = jnp.clip(jax.random.normal(first_key, (D, V), jnp.float32), -6.0, 6.0) * (3.0 / math.sqrt(D))
    return jnp.clip(values, -24.0, 24.0).astype(jnp.bfloat16)


def draw_doc_ids(key, part):
    holders = TOKENS // TOK_DEV
    device_keys = jax.random.split(jax.random.fold_in(key, 11), holders)

    def starts_of(one_key):
        order = jax.random.permutation(one_key, TOK_DEV - 1) + 1
        return order[:DOC_DEV].astype(jnp.int32)
    starts = jax.vmap(starts_of)(device_keys)
    starts = starts.at[0, 0].set(0)
    device_rows = jnp.arange(holders, dtype=jnp.int32)[:, None]
    flags = jnp.zeros((holders, TOK_DEV), jnp.int32).at[device_rows, starts].set(1)
    runs = jnp.cumsum(flags.reshape(-1)) - 1
    return runs.astype(jnp.int32)


def plant(array, key, low, largest):
    shape = array.shape
    spot = [jax.random.randint(jax.random.fold_in(key, axis), (), 0, shape[axis]) for axis in range(len(shape))]
    array = array.at[tuple(spot)].set(low)
    longest = shape.index(max(shape))
    spot[longest] = (spot[longest] + 1) % shape[longest]
    return array.at[tuple(spot)].set(largest)


def level_of(own_key, dims, cuts, least, largest):
    factor_of, own = 1.0, jax.random.fold_in(own_key, 6)
    for position, parts in cuts:
        steps = jnp.exp(jax.random.uniform(jax.random.fold_in(own, position), (parts,), jnp.float32, least / len(cuts), largest / len(cuts)))
        factor_of = factor_of * jnp.repeat(steps, dims[position] // parts).reshape([-1 if axis == position else 1 for axis in range(len(dims))])
    return factor_of


def cumulative_ranks(count, slope):
    weights = [(1 << 20) // math.isqrt(standing ** slope) + 1 for standing in range(1, count + 1)]
    deviation = 1 + sum(weights) // (1 << 30)
    return np.cumsum(np.array([max(1, weight // deviation) for weight in weights]))


def ranked(key, shape, amount, slope):
    listing = cumulative_ranks(amount, slope)
    pick = jax.random.randint(jax.random.fold_in(key, 1), shape, 0, int(listing[amount - 1]))
    standing = jnp.searchsorted(jnp.asarray(listing, jnp.int32), pick, side="right")
    return jax.random.permutation(jax.random.fold_in(key, 2), amount)[standing].astype(jnp.int32)


def assign_block(own_key, own, number, rows, number_of, top, reach, skew):
    sequence = jax.random.permutation(own_key, number_of)
    crowded, ordinary = shares(number_of, rows * top, reach, skew, True), shares(number_of, rows * top, reach, skew, False)
    places = jnp.arange(number_of)

    def named(tallies, offset_by):
        used = int((tallies > 0).sum())
        fixed = max(1, used // 4)
        moved = fixed + (places - fixed + offset_by * (used - fixed)) % max(1, number_of - fixed)
        return jnp.zeros((number_of,), jnp.int32).at[sequence[jnp.where(places < fixed, places, moved)]].set(jnp.asarray(tallies, jnp.int32))

    tallies = jnp.where(number % 4 == 0, named(crowded, number // 4), named(ordinary, number - number // 4 - 1))
    mixed = jax.random.permutation(jax.random.fold_in(own, 3), number_of)
    source_of, receiver = mixed[0:number_of // 2 * 2:2], mixed[1:number_of // 2 * 2:2]
    slack = jnp.minimum(tallies[source_of] - 1, reach - tallies[receiver]) // 2
    slack = jnp.where((source_of == sequence[0]) | (receiver == sequence[0]) | (tallies[receiver] == 0), 0, jnp.maximum(slack, 0))
    moved = jax.random.randint(jax.random.fold_in(own, 4), (number_of // 2,), 0, 1 << 20) % (slack + 1)
    tallies = tallies.at[source_of].add(-moved).at[receiver].add(moved)
    members = jnp.searchsorted(jnp.cumsum(tallies), jnp.arange(rows * top), side="right").astype(jnp.int32)
    table = members.reshape(top, rows).T
    table = table[jax.random.permutation(jax.random.fold_in(own, 1), rows)]
    offset_by = jax.random.randint(jax.random.fold_in(own, 2), (rows, 1), 0, top)
    return jnp.take_along_axis(table, (jnp.arange(top)[None, :] + offset_by) % top, axis=1)


def shares(count, total, limit, lean, full):
    weights = [(1 << 20) // math.isqrt(standing ** lean) + 1 for standing in range(1, count + 1)]
    largest = limit if full else min(limit, max(-(-total // count), total * weights[0] // sum(weights)))
    least = 1 if total - largest >= count - 1 else 0
    given, rest = [largest] + [least] * (count - 1), total - largest - least * (count - 1)
    while rest > 0:
        movable = [i for i in range(1, count) if given[i] < largest] or [i for i in range(1, count) if given[i] < limit]
        mass, budget = sum([weights[i] for i in movable]), rest
        for i in movable:
            extra = min(limit - given[i], max(1, budget * weights[i] // mass), rest)
            given[i] = given[i] + extra
            rest = rest - extra
    return np.array(given)


def centred(stream_key, extent, spread, reach, shards=(), kind=jnp.bfloat16):
    drawn = spread * jax.random.normal(stream_key, extent, jnp.float32)
    if shards:
        drawn = drawn * level_of(stream_key, extent, shards, -0.22, 0.18)
    return jnp.clip(drawn, -reach, reach).astype(kind)


def setup_inputs(seed: int = 0) -> dict:
    streams_of = jax.random.split(jax.random.key(seed), 12)
    hidden_in = centred(streams_of[0], (TOKENS, D), 1.0, 6.0, ((0, 32),))
    moe_gain = jnp.clip(1.0 + 0.18 * jax.random.normal(streams_of[1], (D,), jnp.float32), 0.1, 1.9)
    router_weight = centred(streams_of[2], (D, E), D ** -0.5, 0.1875)
    expert_gate = centred(streams_of[3], (E, D, FF), D ** -0.5, 0.1875, ((0, 8),))
    expert_up = centred(streams_of[4], (E, D, FF), D ** -0.5, 0.1875, ((0, 8),))
    expert_down = centred(streams_of[5], (E, FF, D), FF ** -0.5, 0.1875, ((0, 8),))
    final_gain = jnp.clip(1.0 + 0.18 * jax.random.normal(streams_of[6], (D,), jnp.float32), 0.1, 1.9)
    vocab_weight = draw_vocab_weight(jax.random.fold_in(streams_of[11], 71), 0)
    token_ids = plant(ranked(streams_of[8], (TOKENS,), V, 2), jax.random.fold_in(streams_of[8], 3), 0, V - 1).astype(jnp.int32)
    doc_ids = draw_doc_ids(jax.random.fold_in(streams_of[11], 71), 0)
    routes_keys = jax.random.split(jax.random.fold_in(streams_of[10], 1), TOKENS // TOK_DEV)
    routes_turns = jax.random.permutation(jax.random.fold_in(streams_of[10], 3), TOKENS // TOK_DEV)
    routes = jax.vmap(lambda own, number: assign_block(jax.random.fold_in(streams_of[10], 2), own, number, TOK_DEV, E, TOP, CAP, 2))(routes_keys, routes_turns).reshape((TOKENS, TOP))
    return dict(hidden_in=hidden_in, moe_gain=moe_gain, router_weight=router_weight, expert_gate=expert_gate, expert_up=expert_up, expert_down=expert_down, final_gain=final_gain, vocab_weight=vocab_weight, token_ids=token_ids, doc_ids=doc_ids, routes=routes)


EPSILON = 1e-06

def normalize(values, gain_vector):
    inv_scale = lax.rsqrt(lax.optimization_barrier(jnp.mean(values * values, axis=-1, keepdims=True)) + EPSILON)
    return values * inv_scale * gain_vector

def reference(hidden_in, moe_gain, router_weight, expert_gate, expert_up, expert_down, final_gain, vocab_weight, token_ids, doc_ids, routes):
    devices = N_DP * N_EXPERT
    residual = hidden_in.astype(jnp.float32)
    normed = normalize(residual, moe_gain).astype(jnp.bfloat16)
    router_scores = jnp.dot(normed, router_weight, preferred_element_type=jnp.float32)
    picked_scores = jnp.take_along_axis(router_scores, routes, axis=1)
    first_gate = jax.nn.sigmoid(picked_scores[:, 0] - picked_scores[:, 1])
    second_gate = 1.0 - first_gate
    flat_routes = routes.reshape(devices, TOK_DEV * TOP)
    one_hot = (flat_routes[:, :, None] == jnp.arange(E, dtype=jnp.int32)[None, None, :]).astype(jnp.int32)
    slot_index = lax.optimization_barrier(jnp.sum(one_hot * jnp.cumsum(one_hot, axis=1), axis=-1)) - 1
    source = jnp.arange(devices, dtype=jnp.int32)[:, None]
    target_slot = (flat_routes * (devices * CAP) + source * CAP + slot_index).reshape(-1).astype(jnp.int32)
    repeated = jnp.repeat(normed, TOP, axis=0)
    buffer = jnp.zeros((E * devices * CAP, D), jnp.bfloat16).at[target_slot].set(repeated)

    def run_expert(packed):
        inputs, weight_gate, weight_up, weight_down = packed
        gate_part = jnp.dot(inputs, weight_gate, preferred_element_type=jnp.float32)
        up_part = jnp.dot(inputs, weight_up, preferred_element_type=jnp.float32)
        active = (jax.nn.silu(gate_part) * up_part).astype(jnp.bfloat16)
        return jnp.dot(active, weight_down, preferred_element_type=jnp.float32).astype(jnp.bfloat16)
    results = lax.map(run_expert, (buffer.reshape(E, devices * CAP, D), expert_gate, expert_up, expert_down))
    outputs = results.reshape(E * devices * CAP, D)[target_slot].reshape(TOKENS, TOP, D).astype(jnp.float32)
    mixed = residual + (first_gate[:, None] * outputs[:, 0, :] + second_gate[:, None] * outputs[:, 1, :])
    final_rows = normalize(mixed, final_gain).astype(jnp.bfloat16)
    targets = jnp.concatenate([token_ids[1:], jnp.zeros((1,), jnp.int32)]).astype(jnp.int32)
    following = jnp.concatenate([doc_ids[1:], jnp.full((1,), -1, jnp.int32)])
    counted = following == doc_ids

    def head_block(packed):
        block_rows, block_targets = packed
        scores = jnp.dot(block_rows, vocab_weight, preferred_element_type=jnp.float32)
        highest = lax.optimization_barrier(jnp.max(scores, axis=1))
        log_norm = highest + jnp.log(lax.optimization_barrier(jnp.sum(jnp.exp(scores - highest[:, None]), axis=1)))
        target_score = jnp.take_along_axis(scores, block_targets[:, None], axis=1)[:, 0]
        return log_norm - target_score
    differences = lax.map(head_block, (final_rows.reshape(devices, TOK_DEV, D), targets.reshape(devices, TOK_DEV))).reshape(TOKENS)
    token_loss = jnp.where(counted, differences, jnp.zeros_like(differences))
    doc_loss = jax.ops.segment_sum(token_loss, doc_ids, num_segments=DOCS)
    doc_length = jax.ops.segment_sum(jnp.ones_like(token_loss), doc_ids, num_segments=DOCS)
    global_mean = jnp.sum(token_loss) / (TOKENS - DOCS)
    doc_score = doc_loss / doc_length - global_mean
    return (token_loss, doc_score)
```

```python
import functools

import jax
import jax.numpy as jnp
from jax import lax
from jax.experimental import pallas as pl
from jax.experimental.pallas import tpu as pltpu
from jax.sharding import PartitionSpec as P

TOP = 2
DOC_DEV = 4
CORES = 2
EPSILON = 1e-06
LANES = 128
LOWEST = -3.0e38


BOTH = ("dp", "expert")
VMEM_WHOLE = pl.BlockSpec(memory_space=pltpu.VMEM)


def sibling(value):
    count = lax.axis_size("expert")
    return lax.ppermute(value, "expert", [(i, i ^ 1) for i in range(count)])


def ring(value, steps):
    count = lax.axis_size("expert")
    return lax.ppermute(
        value, "expert", [(i, (i + CORES * steps) % count) for i in range(count)]
    )


def ring_gather(block):
    half = lax.axis_size("expert") // CORES // 2
    up = down = block
    near = [block]
    for _ in range(half - 1):
        up, down = ring(up, 1), ring(down, -1)
        near += [up, down]
    return near


def last_hop(up, down):
    count = lax.axis_size("expert")
    middle = count // CORES // 2 * CORES
    up = lax.ppermute(up, "expert", [(i - CORES, i) for i in range(middle, count)])
    down = lax.ppermute(down, "expert", [(i + CORES, i) for i in range(middle)])
    return up, down


def ring_scatter(parts):
    count = lax.axis_size("expert")
    half = count // CORES // 2
    middle = CORES * half
    up = lax.ppermute(parts[-1], "expert", [(i, i + CORES) for i in range(middle)])
    down = lax.ppermute(parts[-1], "expert", [(i, i - CORES) for i in range(middle, count)])
    for distance in range(half - 1, 0, -1):
        up = ring(parts[2 * distance] + up, 1)
        down = ring(parts[2 * distance - 1] + down, -1)
    return up, down


def offsets(chips):
    half = chips // 2
    near = [0]
    for distance in range(1, half):
        near += [-distance, distance]
    return near + [half]


def shift_gather(block):
    chips = lax.axis_size("expert") // CORES
    return [block if o == 0 else ring(block, -o) for o in offsets(chips)]


def normalize(values, gain_vector):
    inv_scale = lax.rsqrt(jnp.mean(values * values, axis=-1, keepdims=True) + EPSILON)
    return values * inv_scale * gain_vector


def total(refs):
    value = refs[0][...]
    for ref in refs[1:]:
        value = value + ref[...]
    return value


def prepare_kernel(row_count, experts, slots, *refs):
    row_refs, rest = refs[:row_count], refs[row_count:]
    gain_ref, router_ref, ids_ref, routes_ref, x_ref, place_ref, gate_ref = rest
    normed = normalize(total(row_refs).astype(jnp.float32), gain_ref[...]).astype(jnp.bfloat16)
    tokens = normed.shape[0]
    scores = lax.dot_general(
        router_ref[...], normed, (((1,), (1,)), ((), ())), preferred_element_type=jnp.float32
    )
    first, second = routes_ref[0:1, :], routes_ref[1:2, :]
    names = lax.broadcasted_iota(jnp.int32, scores.shape, 0)
    first_score = jnp.sum(jnp.where(names == first, scores, 0.0), axis=0, keepdims=True)
    second_score = jnp.sum(jnp.where(names == second, scores, 0.0), axis=0, keepdims=True)
    first_gate = jax.nn.sigmoid(first_score - second_score)
    second_gate = 1.0 - first_gate
    ids = ids_ref[...]
    is_first = ids == first
    chosen = is_first | (ids == second)
    earlier = lax.broadcasted_iota(jnp.int32, (tokens, tokens), 0)
    later = lax.broadcasted_iota(jnp.int32, (tokens, tokens), 1)
    counts = jnp.dot(
        jnp.where(chosen, 1.0, 0.0).astype(jnp.bfloat16),
        jnp.where(earlier <= later, 1.0, 0.0).astype(jnp.bfloat16),
        preferred_element_type=jnp.float32,
    )
    position = jnp.where(chosen, counts, 0.0).astype(jnp.int32) - 1
    gates = jnp.where(is_first, first_gate, second_gate)
    slot = lax.broadcasted_iota(jnp.int32, (slots, tokens), 0)
    for e in range(experts):
        hit = position[e : e + 1, :] == slot
        part = pl.ds(e * slots, slots)
        place_ref[part, :] = jnp.where(hit, 1.0, 0.0).astype(jnp.bfloat16)
        gate = jnp.sum(jnp.where(hit, gates[e : e + 1, :], 0.0), axis=1, keepdims=True)
        gate_ref[part, :] = jnp.broadcast_to(gate, (slots, LANES))
    x_ref[...] = jnp.dot(place_ref[...], normed, preferred_element_type=jnp.float32).astype(
        jnp.bfloat16
    )


def prepare(rows, gain, router_t, ids, routes, slots, experts):
    tokens, width = rows[0].shape
    filled = experts * slots
    return pl.pallas_call(
        functools.partial(prepare_kernel, len(rows), experts, slots),
        out_shape=(
            jax.ShapeDtypeStruct((filled, width), jnp.bfloat16),
            jax.ShapeDtypeStruct((filled, tokens), jnp.bfloat16),
            jax.ShapeDtypeStruct((filled, LANES), jnp.float32),
        ),
        in_specs=[VMEM_WHOLE] * (len(rows) + 4),
        out_specs=(VMEM_WHOLE,) * 3,
        cost_estimate=pl.CostEstimate(
            flops=2 * filled * tokens * width,
            bytes_accessed=2 * (tokens + filled) * width,
            transcendentals=0,
        ),
        name="prepare",
    )(*rows, gain, router_t, ids, routes)


def expert_kernel(groups, local, slots, tiles, *refs):
    x_refs, refs = refs[:groups], refs[groups:]
    place_refs, refs = refs[:groups], refs[groups:]
    gate_refs, refs = refs[:groups], refs[groups:]
    own_refs, sib_refs, refs = refs[:3], refs[3:6], refs[6:]
    out_refs, (x_all, done, acc) = refs[:groups], refs[groups:]
    expert, tile = pl.program_id(0), pl.program_id(1)
    experts = 2 * local

    @pl.when((expert == 0) & (tile == 0))
    def _():
        for e in range(experts):
            for s in range(groups):
                x_all[e, pl.ds(s * slots, slots), :] = x_refs[s][pl.ds(e * slots, slots), :]

    def step(weights):
        gate_w, up_w, down_w = weights
        x = x_all[expert]
        gate = jnp.dot(x, gate_w[0], preferred_element_type=jnp.float32)
        up = jnp.dot(x, up_w[0], preferred_element_type=jnp.float32)
        active = (jax.nn.silu(gate) * up).astype(jnp.bfloat16)
        part = jnp.dot(active, down_w[0], preferred_element_type=jnp.float32)

        @pl.when(tile == 0)
        def _():
            acc[...] = part

        @pl.when(tile > 0)
        def _():
            acc[...] += part

    @pl.when(expert < local)
    def _():
        step(own_refs)

    @pl.when(expert >= local)
    def _():
        step(sib_refs)

    @pl.when(tile == tiles - 1)
    def _():
        for s in range(groups):
            at = pl.multiple_of(expert * slots, slots)
            gate = gate_refs[s][pl.ds(at, slots), 0:1]
            done[s, pl.ds(at, slots), :] = (acc[pl.ds(s * slots, slots), :] * gate).astype(
                jnp.bfloat16
            )

    @pl.when((expert == experts - 1) & (tile == tiles - 1))
    def _():
        for s in range(groups):
            out_refs[s][...] = lax.dot_general(
                place_refs[s][...],
                done[s],
                (((0,), (0,)), ((), ())),
                preferred_element_type=jnp.float32,
            ).astype(jnp.bfloat16)


def run_experts(prepared, own, sib, slots, tokens):
    groups = len(prepared)
    local, width, hidden = own[0].shape
    experts = 2 * local
    tile = min(512, hidden)
    tiles = hidden // tile

    def wide(side):
        if side == 0:
            return pl.BlockSpec(
                (1, width, tile),
                lambda e, f: (jnp.minimum(e, local - 1), 0, jnp.where(e < local, f, tiles - 1)),
            )
        return pl.BlockSpec(
            (1, width, tile), lambda e, f: (jnp.maximum(e - local, 0), 0, jnp.where(e < local, 0, f))
        )

    def tall(side):
        if side == 0:
            return pl.BlockSpec(
                (1, tile, width),
                lambda e, f: (jnp.minimum(e, local - 1), jnp.where(e < local, f, tiles - 1), 0),
            )
        return pl.BlockSpec(
            (1, tile, width), lambda e, f: (jnp.maximum(e - local, 0), jnp.where(e < local, 0, f), 0)
        )

    flat = [p[0] for p in prepared] + [p[1] for p in prepared] + [p[2] for p in prepared]
    out = pl.pallas_call(
        functools.partial(expert_kernel, groups, local, slots, tiles),
        grid=(experts, tiles),
        out_shape=tuple(jax.ShapeDtypeStruct((tokens, width), jnp.bfloat16) for _ in range(groups)),
        in_specs=[VMEM_WHOLE] * len(flat) + [wide(0), wide(0), tall(0), wide(1), wide(1), tall(1)],
        out_specs=(VMEM_WHOLE,) * groups,
        scratch_shapes=[
            pltpu.VMEM((experts, groups * slots, width), jnp.bfloat16),
            pltpu.VMEM((groups, experts * slots, width), jnp.bfloat16),
            pltpu.VMEM((groups * slots, width), jnp.float32),
        ],
        cost_estimate=pl.CostEstimate(
            flops=6 * experts * groups * slots * width * hidden,
            bytes_accessed=6 * experts * width * hidden,
            transcendentals=0,
        ),
        compiler_params=pltpu.CompilerParams(vmem_limit_bytes=61 * 2**20),
        name="experts",
    )(*flat, *own, *sib)
    return list(out)


def head_kernel(shape, tiles, *refs):
    row_refs = []
    for members in shape:
        row_refs.append(refs[:members])
        refs = refs[members:]
    base_ref, target_ref, own_ref, sib_ref, out_ref, rows, high, sums, picked = refs
    step = pl.program_id(0)
    tokens = row_refs[0][0].shape[0]
    width = own_ref.shape[1]

    @pl.when(step == 0)
    def _():
        for g, members in enumerate(row_refs):
            rows[pl.ds(g * tokens, tokens), :] = total(members)
        high[...] = jnp.full_like(high, LOWEST)
        sums[...] = jnp.zeros_like(sums)
        picked[...] = jnp.zeros_like(picked)

    lane = lax.broadcasted_iota(jnp.int32, (rows.shape[0], LANES), 1)
    wanted = target_ref[...] - step * width - lane

    def add(scores, base):
        pieces = [scores[:, k * LANES : (k + 1) * LANES] for k in range(width // LANES)]
        before = high[...]
        now = jnp.maximum(before, functools.reduce(jnp.maximum, pieces))
        added = sums[...] * jnp.exp(before - now)
        sums[...] = added + sum(jnp.exp(piece - now) for piece in pieces)
        found = picked[...]
        here = wanted - base
        for k, piece in enumerate(pieces):
            found = found + jnp.where(here == k * LANES, piece, 0.0)
        picked[...] = found
        high[...] = now

    own = jnp.dot(rows[...], own_ref[...], preferred_element_type=jnp.float32)
    sib = jnp.dot(rows[...], sib_ref[...], preferred_element_type=jnp.float32)
    add(own, base_ref[0])
    add(sib, base_ref[1])

    @pl.when(step == tiles - 1)
    def _():
        lanes_high = high[...]
        highest = jnp.max(lanes_high, axis=1, keepdims=True)
        sum_all = jnp.sum(sums[...] * jnp.exp(lanes_high - highest), axis=1, keepdims=True)
        log_sum = highest + jnp.log(sum_all)
        found = jnp.sum(picked[...], axis=1, keepdims=True)
        lane = lax.broadcasted_iota(jnp.int32, lanes_high.shape, 1)
        both = jnp.where(lane == 0, log_sum, found)
        out_ref[...] = jnp.transpose(both)[0:8, :]


def head(groups, bases, targets, own, sib):
    tokens, width = groups[0][0].shape
    shape = tuple(len(g) for g in groups)
    many = tokens * len(groups)
    entries = own.shape[1]
    tile = min(1024, entries)
    tiles = entries // tile
    flat = [a for g in groups for a in g]
    out = pl.pallas_call(
        functools.partial(head_kernel, shape, tiles),
        grid=(tiles,),
        out_shape=jax.ShapeDtypeStruct((8, many), jnp.float32),
        in_specs=[VMEM_WHOLE] * len(flat)
        + [pl.BlockSpec(memory_space=pltpu.SMEM), VMEM_WHOLE]
        + [
            pl.BlockSpec((width, tile), lambda j: (0, j)),
            pl.BlockSpec((width, tile), lambda j: (0, j)),
        ],
        out_specs=VMEM_WHOLE,
        scratch_shapes=[pltpu.VMEM((many, width), jnp.bfloat16)]
        + [pltpu.VMEM((many, LANES), jnp.float32)] * 3,
        cost_estimate=pl.CostEstimate(
            flops=4 * many * width * entries,
            bytes_accessed=4 * width * entries,
            transcendentals=2 * many * entries,
        ),
        compiler_params=pltpu.CompilerParams(vmem_limit_bytes=61 * 2**20),
        name="head",
    )(*flat, bases, targets, own, sib)
    return out[0:2]


def finish_kernel(chips, order, *refs):
    early_refs, refs = refs[:chips], refs[chips:]
    late_refs, refs = refs[:chips], refs[chips:]
    number_refs, refs = refs[:chips], refs[chips:]
    docs_ref, start_ref, loss_ref, packed_ref = refs
    everything = jnp.zeros((1, 1), jnp.float32)
    for group in range(chips):
        logs, picks = [], []
        for sender, place in order[group * chips : (group + 1) * chips]:
            ref, row = (late_refs[sender], 0) if place == chips - 1 else (early_refs[sender], 2 * place)
            logs.append(ref[row : row + 1, :])
            picks.append(ref[row + 1 : row + 2, :])
        highest = functools.reduce(jnp.maximum, logs)
        log_norm = highest + jnp.log(sum(jnp.exp(value - highest) for value in logs))
        loss = jnp.where(number_refs[group][1:2, :] == 1, log_norm - sum(picks), 0.0)
        everything = everything + jnp.sum(loss, axis=1, keepdims=True)
        if group == 0:
            own = loss
    loss_ref[...] = own
    docs = docs_ref[...] - start_ref[0]
    tall = (8, docs.shape[1])
    mine = docs == lax.broadcasted_iota(jnp.int32, tall, 0)
    wide = (8, LANES)
    row = lax.broadcasted_iota(jnp.int32, wide, 0)
    lane = lax.broadcasted_iota(jnp.int32, wide, 1)

    def across(column):
        return jnp.sum(jnp.where(lane == row, column, 0.0), axis=0, keepdims=True)

    doc_loss = across(jnp.sum(jnp.where(mine, own, 0.0), axis=1, keepdims=True))
    doc_length = across(jnp.sum(jnp.where(mine, 1.0, 0.0), axis=1, keepdims=True))
    lead_loss = jnp.sum(jnp.where(docs < 0, own, 0.0), axis=1, keepdims=True)
    lead_length = jnp.sum(jnp.where(docs < 0, 1.0, 0.0), axis=1, keepdims=True)
    last = lane == DOC_DEV - 1
    packed = jnp.where(row == 0, everything, 0.0)
    packed = jnp.where(row == 1, doc_loss, packed)
    packed = jnp.where(row == 2, doc_length, packed)
    packed = jnp.where((row == 3) & last, lead_loss, packed)
    packed_ref[...] = jnp.where((row == 4) & last, lead_length, packed)


def finish(early, late, numbers, docs, doc_start, order):
    chips = len(early)
    flat = list(early) + list(late) + list(numbers) + [docs]
    return pl.pallas_call(
        functools.partial(finish_kernel, chips, order),
        out_shape=(
            jax.ShapeDtypeStruct(docs.shape, jnp.float32),
            jax.ShapeDtypeStruct((8, LANES), jnp.float32),
        ),
        in_specs=[VMEM_WHOLE] * len(flat) + [pl.BlockSpec(memory_space=pltpu.SMEM)],
        out_specs=(VMEM_WHOLE, VMEM_WHOLE),
        name="finish",
    )(*flat, doc_start)


def local(
    hidden_in,
    moe_gain,
    router_weight,
    expert_gate,
    expert_up,
    expert_down,
    final_gain,
    vocab_weight,
    token_ids,
    doc_ids,
    routes,
):
    tok_rows, width = hidden_in.shape
    owners = lax.axis_size("expert")
    replicas = lax.axis_size("dp")
    chips = owners // CORES
    local_experts = expert_gate.shape[0]
    experts = owners * local_experts
    slots = max(2, 2 * TOP * tok_rows // experts)
    me = lax.axis_index("expert")
    both = jnp.stack([me, me ^ 1])
    devices = replicas * owners
    assert owners % (2 * CORES) == 0 and replicas & (replicas - 1) == 0
    number = lax.axis_index("dp") * owners + me

    near = ring_gather(hidden_in)
    own_experts = (expert_gate, expert_up, expert_down)
    sib_experts = tuple(sibling(w) for w in own_experts)
    sib_vocab = sibling(vocab_weight)

    routed = shift_gather(routes.T)
    first_pair = jnp.stack([token_ids[0], doc_ids[0]])
    following = lax.ppermute(first_pair, BOTH, [(i, i - 1) for i in range(1, devices)])
    targets = jnp.concatenate([token_ids[1:], following[:1]])
    counted = jnp.concatenate([doc_ids[1:], following[1:]]) == doc_ids
    numbers = jnp.stack([targets, counted.astype(jnp.int32)])

    ids = (both[:, None] * local_experts + jnp.arange(local_experts)[None, :]).reshape(-1)
    ids = jnp.concatenate([ids, jnp.full((-ids.shape[0] % 8,), -1, jnp.int32)])[:, None]
    gain = moe_gain[None, :]
    router_t = router_weight.T

    def ready(rows, named):
        return prepare(rows, gain, router_t, ids, named, slots, 2 * local_experts)

    first = ready((hidden_in,), routed[0])
    up, down, first = lax.optimization_barrier((near[-2], near[-1], first))
    if chips == 2:
        up = down = hidden_in
    far = last_hop(up, down)
    numbers = shift_gather(numbers)
    prepared = [ready((rows,), named) for rows, named in zip(near[1:], routed[1:])]
    far, prepared, numbers = lax.optimization_barrier((far, prepared, numbers))
    prepared = [first] + prepared + [ready(far, routed[-1])]
    parts = run_experts(prepared, own_experts, sib_experts, slots, tok_rows)
    up, down = ring_scatter(parts)
    mixed = hidden_in.astype(jnp.float32)
    for part in (parts[0], up, down):
        mixed = mixed + part.astype(jnp.float32)
    final_rows = normalize(mixed, final_gain).astype(jnp.bfloat16)

    near = ring_gather(final_rows)
    bases = (both * vocab_weight.shape[1]).astype(jnp.int32)

    def run_head(groups, numbered):
        wanted = jnp.concatenate([n[0] for n in numbered])
        wanted = jnp.broadcast_to(wanted[:, None], (wanted.shape[0], LANES))
        found = head(groups, bases, wanted, vocab_weight, sib_vocab)
        return [found[:, k * tok_rows : (k + 1) * tok_rows] for k in range(len(groups))]

    stats = run_head([(final_rows,)], numbers[:1])
    up, down, stats = lax.optimization_barrier((near[-2], near[-1], stats))
    if chips == 2:
        up = down = final_rows
    far = last_hop(up, down)
    for g in range(1, chips - 1, 2):
        stats += run_head([(near[g],), (near[g + 1],)], numbers[g : g + 2])
    far, stats = lax.optimization_barrier((far, stats))
    stats += run_head([far], numbers[-1:])

    place = {o % chips: g for g, o in enumerate(offsets(chips))}
    early = jnp.concatenate(stats[:-1])
    early = shift_gather(early)
    late = shift_gather(stats[-1])
    senders = offsets(chips)
    order = tuple((k, place[(o - senders[k]) % chips]) for o in senders for k in range(chips))
    doc_start = (number * DOC_DEV).reshape(1)
    token_loss, packed = finish(early, late, numbers, doc_ids[None, :], doc_start, order)
    lead = lax.ppermute(packed, BOTH, [(i, i - 1) for i in range(1, devices)])
    loss_sum = packed[0:1]
    loss_sum = loss_sum + sibling(loss_sum)
    bit = 1
    while bit < replicas:
        swap = [(i, i ^ bit) for i in range(replicas)]
        loss_sum = loss_sum + lax.ppermute(loss_sum, "dp", swap)
        bit *= 2
    global_mean = loss_sum[0, :DOC_DEV] / (tok_rows * devices - DOC_DEV * devices)
    doc_loss = packed[1, :DOC_DEV] + lead[3, :DOC_DEV]
    doc_length = packed[2, :DOC_DEV] + lead[4, :DOC_DEV]
    doc_score = doc_loss / doc_length - global_mean
    token_loss = token_loss.reshape(tok_rows)
    return (token_loss, doc_score)


def solution(mesh):
    in_specs = (
        P(("dp", "expert"), None),
        P(),
        P(),
        P("expert", None, None),
        P("expert", None, None),
        P("expert", None, None),
        P(),
        P(None, "expert"),
        P(("dp", "expert")),
        P(("dp", "expert")),
        P(("dp", "expert"), None),
    )
    out_specs = (P(("dp", "expert")), P(("dp", "expert")))
    return jax.shard_map(local, mesh=mesh, in_specs=in_specs, out_specs=out_specs, check_vma=False)
```
